32 devices in a mesh: dp: 4 (over y, x), expert: 8 (over z, core).
Axes of the slice: x: 2, y: 2, z: 4, core: 2. Of those that a mesh axis runs over, the one named last changes fastest.
Arguments:
- shortcut_in: bfloat16 [128, 7168], P('expert', 'dp'), may hold values from -6 to 6
- current_in: bfloat16 [128, 7168], P('expert', 'dp'), may hold values from -6 to 6
- expert_ids: int32 [128, 4], P('expert'), may hold values from 0 to 7, all different within a row; in each aligned block of 16 rows (0 to 15, 16 to 31, ...) at most 12 rows name the same one
- route_weight: float32 [128, 4], P('expert'), may hold values from 0.1 to 1
- gate_weight: bfloat16 [8, 7168, 2048], P('expert', 'dp'), may hold values from -0.09375 to 0.09375
- up_weight: bfloat16 [8, 7168, 2048], P('expert', 'dp'), may hold values from -0.09375 to 0.09375
- down_weight: bfloat16 [8, 2048, 7168], P('expert', None, 'dp'), may hold values from -0.125 to 0.125
- shared_gate: bfloat16 [7168, 2048], P('dp'), may hold values from -0.09375 to 0.09375
- shared_up: bfloat16 [7168, 2048], P('dp'), may hold values from -0.09375 to 0.09375
- shared_down: bfloat16 [2048, 7168], P(None, 'dp'), may hold values from -0.125 to 0.125
Outputs:
- mixed: bfloat16 [128, 7168], P('expert', 'dp')
The draws below stay inside these ranges and needn't reach their ends.
Inputs may be any that keep to these rules, and one draw needn't show every extreme that they name: `expert_ids`: each row names 4 different experts. In each aligned block of 16 rows (the tokens of one index of the expert axis) no expert is named by more than 12 rows, and in at least one such block some expert is named by exactly 12 rows.
All inputs are finite; a program needn't handle non-finite values.
Results may differ from the reference program's by a relative error of at most 0.035.
Values may be sent and summed in bfloat16 or wider, within the bound.
A program may use at most 128 MiB of HBM per device.

```python
import math
import jax
import jax.numpy as jnp
import numpy as np
from jax import lax

D = 7168
H = 2048
TOK_DEV = 16
EXPERTS = 8
TOP = 4
CAP = 12
TOKENS = 128
N_DP = 4
N_EXPERT = 8


def strengthened(array, own_key, source, target, parts, factor):
    owner, partner = [(jnp.arange(array.shape[dim]) // (array.shape[dim] // parts)).reshape([-1 if axis == dim else 1 for axis in range(array.ndim)]) for dim in (source, target)]
    chosen = jax.random.permutation(own_key, parts)[partner]
    strong = (owner == chosen) | (owner == (partner + parts // 2) % parts)
    return jnp.where(strong, factor * array, array)


def shard_levels(key, shape, cuts, least, top_value):
    factor_of, own = 1.0, jax.random.fold_in(key, 6)
    for position, blocks in cuts:
        heights = jnp.exp(jax.random.uniform(jax.random.fold_in(own, position), (blocks,), jnp.float32, least / len(cuts), top_value / len(cuts)))
        factor_of = factor_of * jnp.repeat(heights, shape[position] // blocks).reshape([-1 if axis == position else 1 for axis in range(len(shape))])
    return factor_of


def routed_block(own_key, own, number, rows, amount, top, bound, skew):
    sequence = jax.random.permutation(own_key, amount)
    crowded, common = portions_of(amount, rows * top, bound, skew, True), portions_of(amount, rows * top, bound, skew, False)
    places = jnp.arange(amount)

    def named(tallies, offset_by):
        used = int((tallies > 0).sum())
        fixed = max(1, used // 4)
        shifted = fixed + (places - fixed + offset_by * (used - fixed)) % max(1, amount - fixed)
        return jnp.zeros((amount,), jnp.int32).at[sequence[jnp.where(places < fixed, places, shifted)]].set(jnp.asarray(tallies, jnp.int32))

    tallies = jnp.where(number % 4 == 0, named(crowded, number // 4), named(common, number - number // 4 - 1))
    mixed = jax.random.permutation(jax.random.fold_in(own, 3), amount)
    donor, taker = mixed[0:amount // 2 * 2:2], mixed[1:amount // 2 * 2:2]
    slack = jnp.minimum(tallies[donor] - 1, bound - tallies[taker]) // 2
    slack = jnp.where((donor == sequence[0]) | (taker == sequence[0]) | (tallies[taker] == 0), 0, jnp.maximum(slack, 0))
    shifted = jax.random.randint(jax.random.fold_in(own, 4), (amount // 2,), 0, 1 << 20) % (slack + 1)
    tallies = tallies.at[donor].add(-shifted).at[taker].add(shifted)
    labels = jnp.searchsorted(jnp.cumsum(tallies), jnp.arange(rows * top), side="right").astype(jnp.int32)
    listing = labels.reshape(top, rows).T
    listing = listing[jax.random.permutation(jax.random.fold_in(own, 1), rows)]
    offset_by = jax.random.randint(jax.random.fold_in(own, 2), (rows, 1), 0, top)
    return jnp.take_along_axis(listing, (jnp.arange(top)[None, :] + offset_by) % top, axis=1)


def portions_of(number_of, total, reach, skew, full):
    loads = [(1 << 20) // math.isqrt(grade ** skew) + 1 for grade in range(1, number_of + 1)]
    largest = reach if full else min(reach, max(-(-total // number_of), total * loads[0] // sum(loads)))
    least = 1 if total - largest >= number_of - 1 else 0
    given, surplus = [largest] + [least] * (number_of - 1), total - largest - least * (number_of - 1)
    while surplus > 0:
        movable = [i for i in range(1, number_of) if given[i] < largest] or [i for i in range(1, number_of) if given[i] < reach]
        mass, remaining = sum([loads[i] for i in movable]), surplus
        for i in movable:
            extra = min(reach - given[i], max(1, remaining * loads[i] // mass), surplus)
            given[i] = given[i] + extra
            surplus = surplus - extra
    return np.array(given)


def bell_draw(own_key, shape, spread, most, cuts=(), kind=jnp.bfloat16):
    gain = shard_levels(own_key, shape, cuts, -0.22, 0.18) if cuts else 1.0
    entries = jax.random.normal(own_key, shape, jnp.float32) * spread * gain
    return jnp.minimum(jnp.maximum(entries, -most), most).astype(kind)


def bell_draw_with(rng, shape, width, bound, cuts, heavy, kind=jnp.bfloat16):
    array = width * jax.random.normal(rng, shape, jnp.float32)
    if cuts:
        array = array * shard_levels(rng, shape, cuts, -0.22, 0.18)
    return jnp.clip(strengthened(array, jax.random.fold_in(rng, 3), *heavy), -bound, bound).astype(kind)


def setup_inputs(seed: int = 0) -> dict:
    key_list = jax.random.split(jax.random.key(seed), 11)
    shortcut_in = bell_draw(key_list[0], (TOKENS, D), 1.0, 6.0, ((0, 8), (1, 4)))
    current_in = bell_draw(key_list[1], (TOKENS, D), 1.0, 6.0, ((0, 8), (1, 4)))
    expert_ids_keys = jax.random.split(jax.random.fold_in(key_list[2], 1), TOKENS // TOK_DEV)
    expert_ids_turns = jax.random.permutation(jax.random.fold_in(key_list[2], 3), TOKENS // TOK_DEV)
    expert_ids = jax.vmap(lambda own, number: routed_block(jax.random.fold_in(key_list[2], 2), own, number, TOK_DEV, EXPERTS, TOP, CAP, 2))(expert_ids_keys, expert_ids_turns).reshape((TOKENS, TOP))
    route_weight = jnp.clip(jnp.exp(math.log(1.0) - 2.3025851 * jax.random.uniform(key_list[3], (TOKENS, TOP), jnp.float32) ** shard_levels(key_list[3], (TOKENS, TOP), ((0, 8),), -0.2, 0.2)), 0.1, 1.0)
    gate_weight = bell_draw_with(key_list[4], (EXPERTS, D, H), D ** -0.5, 0.09375, ((0, 8), (1, 4)), (1, 2, 4, 2.0))
    up_weight = bell_draw_with(key_list[5], (EXPERTS, D, H), D ** -0.5, 0.09375, ((0, 8), (1, 4)), (1, 2, 4, 2.0))
    down_weight = bell_draw(key_list[6], (EXPERTS, H, D), H ** -0.5, 0.125, ((0, 8), (2, 4)))
    shared_gate = bell_draw_with(key_list[7], (D, H), D ** -0.5, 0.09375, ((0, 4),), (0, 1, 4, 2.0))
    shared_up = bell_draw_with(key_list[8], (D, H), D ** -0.5, 0.09375, ((0, 4),), (0, 1, 4, 2.0))
    shared_down = bell_draw(key_list[9], (H, D), H ** -0.5, 0.125, ((1, 4),))
    return {"shortcut_in": shortcut_in, "current_in": current_in, "expert_ids": expert_ids, "route_weight": route_weight, "gate_weight": gate_weight, "up_weight": up_weight, "down_weight": down_weight, "shared_gate": shared_gate, "shared_up": shared_up, "shared_down": shared_down}


def blocked_product(inputs, weight):
    count = inputs.shape[0]
    block = inputs.shape[1] // N_DP
    pieces = inputs.astype(jnp.float32).reshape(count, N_DP, block)
    blocks = weight.astype(jnp.float32).reshape(N_DP, block, weight.shape[1])
    partial_value = jnp.einsum("rnd,ndh->nrh", pieces, blocks, precision=lax.Precision.HIGHEST)
    rounded = lax.optimization_barrier(partial_value.astype(jnp.bfloat16))
    return jnp.sum(rounded.astype(jnp.float32), axis=0)


def swiglu_hidden(inputs, gate_w, up_w):
    gate = blocked_product(inputs, gate_w)
    upper = blocked_product(inputs, up_w)
    return (jax.nn.silu(gate) * upper).astype(jnp.bfloat16)


def reference(shortcut_in, current_in, expert_ids, route_weight, gate_weight, up_weight, down_weight, shared_gate, shared_up, shared_down):
    count = TOKENS * TOP
    limit = N_EXPERT * CAP
    flat_ids = expert_ids.reshape(-1).astype(jnp.int32)
    flat_tok = jnp.arange(count, dtype=jnp.int32) // TOP
    flat_weight = route_weight.reshape(-1)

    def one_expert(total, inputs):
        gate_w, up_w, down_w, number = inputs
        chosen = flat_ids == number
        rank = jnp.cumsum(chosen.astype(jnp.int32)) - 1
        slots = jnp.where(chosen, rank, limit).astype(jnp.int32)
        source = jnp.zeros((limit,), jnp.int32).at[slots].set(jnp.arange(count, dtype=jnp.int32), mode="drop")
        used = jnp.zeros((limit,), jnp.float32).at[slots].set(1.0, mode="drop")
        token_index = flat_tok[source]
        gathered = shortcut_in[token_index]
        hidden = swiglu_hidden(gathered, gate_w, up_w)
        result = jnp.dot(hidden, down_w, preferred_element_type=jnp.float32).astype(jnp.bfloat16)
        result = lax.optimization_barrier(result).astype(jnp.float32)
        scale = used * flat_weight[source]
        total = total.at[token_index].add(scale[:, None] * result)
        return total, None

    numbers = jnp.arange(EXPERTS, dtype=jnp.int32)
    start = jnp.zeros((TOKENS, D), jnp.float32)
    routed, unused_out = lax.scan(one_expert, start, (gate_weight, up_weight, down_weight, numbers))
    shared_hidden = swiglu_hidden(current_in, shared_gate, shared_up)
    shared_out = jnp.dot(shared_hidden, shared_down, preferred_element_type=jnp.float32)
    return (shared_out + routed).astype(jnp.bfloat16)
```

```python
import functools

import jax
import jax.numpy as jnp
from jax import lax
from jax.experimental import pallas as pl
from jax.experimental.pallas import tpu as pltpu
from jax.sharding import PartitionSpec as P


def activate(summed):
    return (jax.nn.silu(summed[:, 0]) * summed[:, 1]).astype(jnp.bfloat16)


def hidden_of(partial_value):
    summed = lax.psum_scatter(
        partial_value.astype(jnp.bfloat16), "dp", scatter_dimension=2, tiled=True
    ).astype(jnp.float32)
    return lax.all_gather(activate(summed), "dp", axis=1, tiled=True)


def send_rows(outgoing):
    return lax.all_to_all(outgoing, "expert", split_axis=0, concat_axis=0, tiled=True)


def expert_partial(arrived, gate_weight, up_weight):
    gate = jnp.einsum("sacd,adh->sach", arrived, gate_weight, preferred_element_type=jnp.float32)
    upper = jnp.einsum("sacd,adh->sach", arrived, up_weight, preferred_element_type=jnp.float32)
    stacked = jnp.stack([gate, upper], axis=3)
    return stacked.reshape(-1, 2, gate_weight.shape[2])


def local(
    shortcut_in,
    current_in,
    expert_ids,
    route_weight,
    gate_weight,
    up_weight,
    down_weight,
    shared_gate,
    shared_up,
    shared_down,
):
    sources = lax.axis_size("expert")
    local_experts = gate_weight.shape[0]
    experts = sources * local_experts
    tokens, top = expert_ids.shape
    capacity = 3 * tokens * top // (2 * experts)
    width = shortcut_in.shape[1]
    hidden_units = gate_weight.shape[2]
    flat_ids = expert_ids.reshape(-1)
    onehot = (flat_ids[:, None] == jnp.arange(experts, dtype=jnp.int32)[None, :]).astype(jnp.int32)
    rank = jnp.sum((jnp.cumsum(onehot, axis=0) - 1) * onehot, axis=1)
    slot = (flat_ids * capacity + rank).reshape(tokens, top)
    positions = jnp.arange(experts * capacity, dtype=jnp.int32)
    place = jnp.sum((slot[None, :, :] == positions[:, None, None]).astype(jnp.bfloat16), axis=2)
    outgoing = jnp.dot(place, shortcut_in, preferred_element_type=jnp.float32).astype(jnp.bfloat16)
    outgoing = outgoing.reshape(sources, local_experts * capacity, width)
    shared_gate_sum = jnp.dot(current_in, shared_gate, preferred_element_type=jnp.float32)
    shared_up_sum = jnp.dot(current_in, shared_up, preferred_element_type=jnp.float32)
    shared_partial = jnp.stack([shared_gate_sum, shared_up_sum], axis=1)
    routed_rows = experts * capacity
    arrived = send_rows(outgoing).reshape(sources, local_experts, capacity, width)
    routed_partial = expert_partial(arrived, gate_weight, up_weight)
    joined = hidden_of(jnp.concatenate([routed_partial, shared_partial], axis=0))
    routed_hidden = joined[:routed_rows]
    shared_hidden = joined[routed_rows:]
    routed_hidden = routed_hidden.reshape(sources, local_experts, capacity, hidden_units)
    expert_out = jnp.einsum(
        "sach,ahd->sacd", routed_hidden, down_weight, preferred_element_type=jnp.float32
    ).astype(jnp.bfloat16)
    returned = lax.all_to_all(
        expert_out.reshape(sources, local_experts * capacity, width),
        "expert",
        split_axis=0,
        concat_axis=0,
        tiled=True,
    )
    picked = returned.reshape(routed_rows, width)[slot]
    routed = jnp.sum(route_weight[:, :, None] * picked.astype(jnp.float32), axis=1)
    shared_out = jnp.dot(shared_hidden, shared_down, preferred_element_type=jnp.float32)
    return (shared_out + routed).astype(jnp.bfloat16)


MESH = pl.DeviceIdType.MESH
BF = jnp.bfloat16
F32 = jnp.float32
PARTS = 2


def dot(a, b):
    return jnp.dot(a, b, preferred_element_type=F32)


def layer_kernel(
    n_dp, n_e, cap, groups, near,
    x_hbm, cur_hbm, ids_hbm, w_hbm, gate_hbm, up_hbm, down_hbm, sg_hbm, su_hbm, sd_hbm,
    out_ref,
    gu_v, down_v, sgu_v, sd_v, ids_v, w_v, flip, xm, cm,
    xc, part, rs_in, hid, acc, shv, sh_part, sh_in, sh_hid, own_sum, contrib, pair_in, fin_out, fin_in,
    in_sem, gu_sem, down_sem, shw_sem,
    snd, x_r, xp_r, c_r, cp_r, rs_s, rs_r, hid_s, hid_r, shp_r, shh_r, pair_r, fin_r,
):
    me_d = lax.axis_index("dp")
    me_e = lax.axis_index("expert")
    zs = n_e // 2
    z, c = me_e // 2, lax.rem(me_e, 2)
    pairs = zs // 2
    p, b = z // 2, lax.rem(z, 2)
    partner = 2 * z + (1 - c)
    tokens, width = x_hbm.shape
    top = ids_hbm.shape[0]
    chunk = gu_v.shape[2] // 2
    hs = chunk * PARTS
    shc = sgu_v.shape[1] // 2
    held = 2 * tokens
    slots = [(q, s) for q in range(PARTS) for s in [*range(n_dp - 1, 0, -1), 0]]

    def start(src, dst, sem):
        copy = pltpu.make_async_copy(src, dst, sem)
        copy.start()
        return copy

    def landed(dst, sem):
        pltpu.make_async_copy(dst, dst, sem).wait()

    ys = n_dp // 2
    y, x = me_d // 2, lax.rem(me_d, 2)
    to_dp = [2 * lax.rem(y + s // 2, ys) + lax.rem(x + s % 2, 2) for s in range(n_dp)]
    from_dp = [2 * lax.rem(y - s // 2 + ys, ys) + lax.rem(x + s % 2, 2) for s in range(n_dp)]
    to_z = [2 * (2 * lax.rem(p + s // 2, pairs) + lax.rem(b + s % 2, 2)) + c for s in range(zs)]
    from_z = [2 * (2 * lax.rem(p - s // 2 + pairs, pairs) + lax.rem(b + s % 2, 2)) + c for s in range(zs)]

    def dp_dev(s):
        return to_dp[s]

    def dp_src(s):
        return from_dp[s]

    def z_dev(s):
        return to_z[s]

    def z_src(s):
        return from_z[s]

    barrier = pltpu.get_barrier_semaphore()
    pl.semaphore_signal(barrier, inc=1, device_id=(me_d, partner), device_id_type=MESH)
    for s in range(1, zs):
        pl.semaphore_signal(barrier, inc=1, device_id=(me_d, z_dev(s)), device_id_type=MESH)
    for s in range(1, n_dp):
        pl.semaphore_signal(barrier, inc=1, device_id=(dp_dev(s), me_e), device_id_type=MESH)

    got_ids = start(ids_hbm, ids_v, in_sem.at[0])
    got_w = start(w_hbm, w_v, in_sem.at[1])
    got_x = start(x_hbm, xm.at[c, :, pl.ds(0, width)], in_sem.at[2])
    got_cur = start(cur_hbm, cm.at[c], in_sem.at[3])
    def fetch_shared():
        mine = pl.ds(pl.multiple_of(lax.rem(me_e, 2 * near) * shc, 128), shc)
        start(sg_hbm.at[:, mine], sgu_v.at[:, pl.ds(0, shc)], shw_sem.at[0])
        start(su_hbm.at[:, mine], sgu_v.at[:, pl.ds(shc, shc)], shw_sem.at[0])
        start(sd_hbm.at[mine, :], sd_v, shw_sem.at[1])

    def fetch_down():
        for q in range(PARTS):
            for i, s in enumerate([*range(n_dp - 1, 0, -1), 0]):
                row = pl.ds(pl.multiple_of(dp_src(s) * hs + q * chunk, 128), chunk)
                start(down_hbm.at[0, row, :], down_v.at[pl.ds((q * n_dp + i) * chunk, chunk), :], down_sem.at[q])

    def remote(src, dst, ssem, rsem, dp, e):
        pltpu.make_async_remote_copy(
            src_ref=src, dst_ref=dst, send_sem=ssem, recv_sem=rsem, device_id=(dp, e), device_id_type=MESH
        ).start()

    before = lax.broadcasted_iota(jnp.int32, (128, 128), 0) < lax.broadcasted_iota(jnp.int32, (128, 128), 1)
    before = jnp.where(before, 1.0, 0.0).astype(BF)
    flip[...] = jnp.zeros_like(flip)
    got_ids.wait()
    got_w.wait()
    flip[:top, :tokens] = ids_v[...].astype(F32)
    flip[top:2 * top, :tokens] = w_v[...]
    named = flip[...]
    named = jnp.where(c == 1, pltpu.roll(named, tokens, 1), named)
    flip[...] = named
    exact = flip[top:2 * top, :]
    first = exact.astype(BF).astype(F32)
    second = (exact - first).astype(BF).astype(F32)
    flip[top:2 * top, :] = first
    flip[2 * top:3 * top, :] = second
    flip[3 * top:4 * top, :] = exact - first - second
    xm[c, :, width:] = flip[...].astype(BF)
    got_x.wait()
    got_cur.wait()
    for i, (q, s) in enumerate(slots):
        col = pl.ds(pl.multiple_of(dp_dev(s) * hs + q * chunk, 128), chunk)
        start(gate_hbm.at[0, :, col], gu_v.at[i, :, pl.ds(0, chunk)], gu_sem.at[i])
        start(up_hbm.at[0, :, col], gu_v.at[i, :, pl.ds(chunk, chunk)], gu_sem.at[i])
    with jax.named_scope("barrier"):
        pl.semaphore_wait(barrier, n_dp - 1 + zs - 1 + 1)

    remote(xm.at[c], xm.at[c], snd.at[0], xp_r.at[0], me_d, partner)
    for s in range(1, zs):
        remote(xm.at[c], xm.at[2 * s + c], snd.at[0], x_r.at[s], me_d, z_dev(s))
    remote(cm.at[c], cm.at[c], snd.at[1], cp_r.at[0], me_d, partner)
    for s in range(1, near):
        remote(cm.at[c], cm.at[2 * s + c], snd.at[1], c_r.at[s], me_d, z_dev(s))

    def relay_x(s):
        with jax.named_scope(f"relay{s}"):
            landed(xm.at[2 * s + c], x_r.at[s])
        remote(xm.at[2 * s + c], xm.at[2 * s + c], snd.at[0], xp_r.at[s], me_d, partner)

    def relay_cur(s):
        with jax.named_scope(f"crelay{s}"):
            landed(cm.at[2 * s + c], c_r.at[s])
        remote(cm.at[2 * s + c], cm.at[2 * s + c], snd.at[1], cp_r.at[s], me_d, partner)

    me_f = me_e.astype(F32)

    def chosen(block):
        table = xm[block, :, width:].astype(F32)
        weight = table[top:2 * top] + table[2 * top:3 * top] + table[3 * top:4 * top]
        return jnp.sum(jnp.where(table[:top] == me_f, weight, 0.0), axis=0, keepdims=True)

    def route(g):
        rows = part[g].shape[1]
        padded = -(-rows // 16) * 16
        for s in groups[g]:
            with jax.named_scope(f"coll{s}"):
                landed(xm.at[2 * s + 1 - c], xp_r.at[s])
        scale = None
        for k, s in enumerate(groups[g]):
            one = chosen(2 * s) + chosen(2 * s + 1)
            one = pltpu.roll(one, held * k, 1) if k else one
            scale = one if scale is None else scale + one
        scale = jnp.broadcast_to(scale, (8, 128))
        rank = dot(jnp.where(scale > 0, 1.0, 0.0).astype(BF), before)[:1]
        scale = scale[:1]
        place = lax.broadcasted_iota(jnp.int32, (padded, 128), 0).astype(F32)
        place = jnp.where(jnp.logical_and(place == rank, scale > 0), 1.0, 0.0)
        size = held * len(groups[g])
        source = jnp.concatenate([xm[2 * s:2 * s + 2, :, :width].reshape(held, width) for s in groups[g]], axis=0)
        xc[g][...] = dot(place[:, :size].astype(BF), source).astype(BF)
        return place, scale

    def gate_up(g, hooks):
        rows = part[g].shape[1]
        for i, (q, s) in enumerate(slots):
            if g == 0:
                with jax.named_scope(f"w{i}"):
                    landed(gu_v.at[i], gu_sem.at[i])
            part[g][i] = dot(xc[g][...], gu_v[i])[:rows].astype(BF)
            if s:
                remote(part[g].at[i], rs_in[g].at[i], rs_s.at[g], rs_r.at[PARTS * g + q], dp_dev(s), me_e)
            for hook in hooks.get(i, ()):
                hook()

    def back(g, place, scale):
        rows = part[g].shape[1]
        size = held * len(groups[g])
        tall = jnp.concatenate([place, jnp.zeros((128 - place.shape[0], 128), F32)], axis=0)
        turned = jnp.transpose(tall)[:size]
        weight = jnp.sum(place * scale, axis=1, keepdims=True)[:rows]
        return turned[:, :rows].astype(BF), weight

    def gated(term, n):
        gate, upper = term[:, :n], term[:, n:]
        return (gate / (1.0 + jnp.exp(-gate)) * upper).astype(BF)

    def act(g, q):
        base = q * n_dp
        others = pl.ds(base, n_dp - 1)
        with jax.named_scope(f"rs{g}{q}"):
            landed(rs_in[g].at[others], rs_r.at[PARTS * g + q])
        term = part[g][base + n_dp - 1].astype(F32)
        for s in range(1, n_dp):
            term = term + rs_in[g][base + n_dp - 1 - s].astype(F32)
        own = base + n_dp - 1
        hid[g][own] = gated(term, chunk)
        for s in range(1, n_dp):
            remote(hid[g].at[own], hid[g].at[base + n_dp - 1 - s], hid_s.at[g], hid_r.at[PARTS * g + q], dp_dev(s), me_e)

    def down(g, weight, between=None):
        span = n_dp * chunk

        def gathered(q):
            with jax.named_scope(f"hid{g}{q}"):
                landed(hid[g].at[pl.ds(q * n_dp, n_dp - 1)], hid_r.at[PARTS * g + q])
            if g == 0:
                landed(down_v.at[pl.ds(q * span, span), :], down_sem.at[q])
            return [hid[g][q * n_dp + i] for i in range(n_dp)]

        rows = part[g].shape[1]
        if between is not None:
            for q in range(PARTS):
                value = dot(jnp.concatenate(gathered(q), axis=1), down_v[q * span:(q + 1) * span])
                if q < PARTS - 1:
                    acc[:rows] = value if q == 0 else acc[:rows] + value
                    between()
            value = acc[:rows] + value
        else:
            pieces = [piece for q in range(PARTS) for piece in gathered(q)]
            value = dot(jnp.concatenate(pieces, axis=1), down_v[...])
        return (weight * value).astype(BF)

    def give(g, turned, value):
        value = dot(turned, value)
        for k, s in enumerate(groups[g]):
            one = value[k * held:(k + 1) * held].reshape(2, tokens, width)
            if s < near:
                one = one + shv[2 * s:2 * s + 2]
            contrib[s] = one.astype(BF)
            remote(contrib.at[s, 1 - c], pair_in.at[s], snd.at[4], pair_r.at[s], me_d, partner)

    def settle(s):
        with jax.named_scope(f"pair{s}"):
            landed(pair_in.at[s], pair_r.at[s])
        summed = contrib[s, c].astype(F32) + pair_in[s].astype(F32)
        if s:
            fin_out[s - 1] = summed.astype(BF)
            remote(fin_out.at[s - 1], fin_in.at[s - 1], snd.at[5], fin_r.at[s], me_d, z_src(s))
        else:
            own_sum[...] = summed

    def shared_up():
        for s in range(near):
            with jax.named_scope(f"ccoll{s}"):
                landed(cm.at[2 * s + 1 - c], cp_r.at[s])
        with jax.named_scope("shw"):
            landed(sgu_v, shw_sem.at[0])
        cur = cm[...].reshape(near * held, width)
        sh_part[...] = dot(cur, sgu_v[...]).astype(BF).reshape(sh_part.shape)
        for s in range(1, n_dp):
            remote(sh_part.at[dp_dev(s)], sh_in.at[s - 1], snd.at[2], shp_r.at[0], dp_dev(s), me_e)

    def shared_act():
        with jax.named_scope("shrs"):
            landed(sh_in, shp_r.at[0])
        term = sh_part[me_d].astype(F32)
        for s in range(1, n_dp):
            term = term + sh_in[s - 1].astype(F32)
        sh_hid[me_d] = gated(term, shc)
        for s in range(1, n_dp):
            remote(sh_hid.at[me_d], sh_hid.at[me_d], snd.at[3], shh_r.at[s], dp_dev(s), me_e)

    def shared_down():
        for s in range(1, n_dp):
            with jax.named_scope(f"shh{s}"):
                landed(sh_hid.at[dp_src(s)], shh_r.at[s])
        landed(sd_v, shw_sem.at[1])
        shv[...] = dot(sh_hid[...].reshape(near * held, shc), sd_v[...]).reshape(shv.shape)

    order = list(range(len(groups)))
    kept = {}

    def do(*calls):
        return [functools.partial(*call) for call in calls]

    hooks = [
        {2: do((fetch_shared,)), 4: do((fetch_down,)), 6: do((relay_x, 1))},
        {2: do((act, 0, 0)), 4: do((act, 0, 1), (relay_x, 2)), 5: do((relay_cur, 1)), 6: do((relay_x, 3))},
        {},
    ]
    for g in order:
        place, scale = route(g)
        gate_up(g, hooks[g])
        kept[g] = back(g, place, scale)
        if g == 1:
            shared_up()
    for q in range(PARTS):
        act(1, q)
    shared_act()
    first_value = down(0, kept[0][1])
    act(2, 0)
    act(2, 1)
    second_value = down(1, kept[1][1])
    shared_down()
    give(0, kept[0][0], first_value)
    give(1, kept[1][0], second_value)

    def near_home():
        settle(1)
        settle(0)

    give(2, kept[2][0], down(2, kept[2][1], near_home))
    settle(3)
    settle(2)
    both = own_sum[...]
    for s in range(1, zs):
        with jax.named_scope(f"fin{s}"):
            landed(fin_in.at[s - 1], fin_r.at[s])
        both = both + fin_in[s - 1].astype(F32)
    out_ref[...] = both.astype(BF)

    def sent(ref, sem):
        pltpu.make_async_remote_copy(
            src_ref=ref, dst_ref=ref, send_sem=sem, recv_sem=sem, device_id=(me_d, partner), device_id_type=MESH
        ).wait_send()

    with jax.named_scope("sendwait"):
        sent(xm.at[pl.ds(0, 2 * zs - 1)], snd.at[0])
        sent(cm.at[pl.ds(0, 2 * near - 1)], snd.at[1])
        sent(sh_part.at[pl.ds(0, n_dp - 1)], snd.at[2])
        sent(sh_hid.at[pl.ds(0, n_dp - 1)], snd.at[3])
        sent(pair_in, snd.at[4])
        sent(fin_out, snd.at[5])
        for g in order:
            sent(part[g].at[pl.ds(0, PARTS * (n_dp - 1))], rs_s.at[g])
            sent(hid[g].at[pl.ds(0, PARTS * (n_dp - 1))], hid_s.at[g])


GROUPS = ((0,), (1,), (2, 3))
NEAR = 2


def fused(n_dp, n_e, shortcut_in, current_in, expert_ids, route_weight, gate_weight, up_weight, down_weight, shared_gate, shared_up, shared_down):
    tokens, width = shortcut_in.shape
    hidden = gate_weight.shape[2]
    top = expert_ids.shape[1]
    cap = 3 * tokens * top // (2 * n_e)
    chunk = hidden // n_dp // PARTS
    count = PARTS * n_dp
    zs = n_e // 2
    shc = hidden // (2 * NEAR)
    share = 2 * NEAR * tokens // n_dp
    rows = [2 * cap * len(g) for g in GROUPS]
    n_g = len(GROUPS)
    V = pltpu.VMEM
    S = pltpu.SemaphoreType.DMA
    scratch = [
        V((count, width, 2 * chunk), BF), V((hidden, width), BF), V((width, 2 * shc), BF), V((shc, width), BF),
        V((top, tokens), jnp.int32), V((top, tokens), F32), V((tokens, 128), F32),
        V((n_e, tokens, width + 128), BF), V((2 * NEAR, tokens, width), BF),
        [V((-(-r // 16) * 16, width), BF) for r in rows], [V((count, r, 2 * chunk), BF) for r in rows], [V((count, r, 2 * chunk), BF) for r in rows], [V((count, r, chunk), BF) for r in rows],
        V((max(rows), width), F32), V((2 * NEAR, tokens, width), F32),
        V((n_dp, share, 2 * shc), BF), V((n_dp - 1, share, 2 * shc), BF), V((n_dp, share, shc), BF), V((tokens, width), F32),
        V((zs, 2, tokens, width), BF), V((zs, tokens, width), BF), V((zs - 1, tokens, width), BF), V((zs - 1, tokens, width), BF),
        S((4,)), S((count,)), S((PARTS,)), S((2,)),
        S((6,)), S((zs,)), S((zs,)), S((NEAR,)), S((NEAR,)),
        S((n_g,)), S((PARTS * n_g,)), S((n_g,)), S((PARTS * n_g,)), S((1,)), S((n_dp,)), S((zs,)), S((zs,)),
    ]
    vm = pl.BlockSpec(memory_space=pltpu.VMEM)
    hbm = pl.BlockSpec(memory_space=pl.ANY)
    return pl.pallas_call(
        functools.partial(layer_kernel, n_dp, n_e, cap, GROUPS, NEAR),
        out_shape=pltpu.VMEM((tokens, width), BF),
        in_specs=[hbm] * 10,
        out_specs=vm,
        scratch_shapes=scratch,
        compiler_params=pltpu.CompilerParams(collective_id=0, has_side_effects=True, vmem_limit_bytes=60 * 1024 * 1024),
    )(shortcut_in, current_in, expert_ids.T, route_weight.T, gate_weight, up_weight, down_weight, shared_gate, shared_up, shared_down)


def body(n_dp, n_e, *arrays):
    tokens, width = arrays[0].shape
    top = arrays[2].shape[1]
    experts, _, hidden = arrays[4].shape
    aligned = (
        experts == 1 and n_e == 2 * sum(len(g) for g in GROUPS) and 4 * top <= tokens and tokens == 16 and width % 128 == 0
        and hidden % (n_dp * PARTS * 128) == 0 and hidden % (2 * NEAR * 128) == 0
        and 2 * NEAR * tokens % (n_dp * 16) == 0 and 3 * tokens * top % (2 * n_e) == 0 and 2 * (3 * tokens * top // (2 * n_e)) % 8 == 0
    )
    return fused(n_dp, n_e, *arrays) if aligned else local(*arrays)


def solution(mesh):
    placed = (
        P("expert", "dp"),
        P("expert", "dp"),
        P("expert", None),
        P("expert", None),
        P("expert", "dp", None),
        P("expert", "dp", None),
        P("expert", None, "dp"),
        P("dp", None),
        P("dp", None),
        P(None, "dp"),
    )
    return jax.shard_map(
        functools.partial(body, mesh.shape["dp"], mesh.shape["expert"]), mesh=mesh, in_specs=placed, out_specs=P("expert", "dp"), check_vma=False
    )
```

```python
import functools

import jax
import jax.numpy as jnp
from jax import lax
from jax.experimental import pallas as pl
from jax.experimental.pallas import tpu as pltpu
from jax.sharding import PartitionSpec as P


def activate(summed):
    return (jax.nn.silu(summed[:, 0]) * summed[:, 1]).astype(jnp.bfloat16)


def hidden_of(partial_value):
    summed = lax.psum_scatter(
        partial_value.astype(jnp.bfloat16), "dp", scatter_dimension=2, tiled=True
    ).astype(jnp.float32)
    return lax.all_gather(activate(summed), "dp", axis=1, tiled=True)


def send_rows(outgoing):
    return lax.all_to_all(outgoing, "expert", split_axis=0, concat_axis=0, tiled=True)


def expert_partial(arrived, gate_weight, up_weight):
    gate = jnp.einsum("sacd,adh->sach", arrived, gate_weight, preferred_element_type=jnp.float32)
    upper = jnp.einsum("sacd,adh->sach", arrived, up_weight, preferred_element_type=jnp.float32)
    stacked = jnp.stack([gate, upper], axis=3)
    return stacked.reshape(-1, 2, gate_weight.shape[2])


def local(
    shortcut_in,
    current_in,
    expert_ids,
    route_weight,
    gate_weight,
    up_weight,
    down_weight,
    shared_gate,
    shared_up,
    shared_down,
):
    sources = lax.axis_size("expert")
    local_experts = gate_weight.shape[0]
    experts = sources * local_experts
    tokens, top = expert_ids.shape
    capacity = 3 * tokens * top // (2 * experts)
    width = shortcut_in.shape[1]
    hidden_units = gate_weight.shape[2]
    flat_ids = expert_ids.reshape(-1)
    onehot = (flat_ids[:, None] == jnp.arange(experts, dtype=jnp.int32)[None, :]).astype(jnp.int32)
    rank = jnp.sum((jnp.cumsum(onehot, axis=0) - 1) * onehot, axis=1)
    slot = (flat_ids * capacity + rank).reshape(tokens, top)
    positions = jnp.arange(experts * capacity, dtype=jnp.int32)
    place = jnp.sum((slot[None, :, :] == positions[:, None, None]).astype(jnp.bfloat16), axis=2)
    outgoing = jnp.dot(place, shortcut_in, preferred_element_type=jnp.float32).astype(jnp.bfloat16)
    outgoing = outgoing.reshape(sources, local_experts * capacity, width)
    shared_gate_sum = jnp.dot(current_in, shared_gate, preferred_element_type=jnp.float32)
    shared_up_sum = jnp.dot(current_in, shared_up, preferred_element_type=jnp.float32)
    shared_partial = jnp.stack([shared_gate_sum, shared_up_sum], axis=1)
    routed_rows = experts * capacity
    arrived = send_rows(outgoing).reshape(sources, local_experts, capacity, width)
    routed_partial = expert_partial(arrived, gate_weight, up_weight)
    joined = hidden_of(jnp.concatenate([routed_partial, shared_partial], axis=0))
    routed_hidden = joined[:routed_rows]
    shared_hidden = joined[routed_rows:]
    routed_hidden = routed_hidden.reshape(sources, local_experts, capacity, hidden_units)
    expert_out = jnp.einsum(
        "sach,ahd->sacd", routed_hidden, down_weight, preferred_element_type=jnp.float32
    ).astype(jnp.bfloat16)
    returned = lax.all_to_all(
        expert_out.reshape(sources, local_experts * capacity, width),
        "expert",
        split_axis=0,
        concat_axis=0,
        tiled=True,
    )
    picked = returned.reshape(routed_rows, width)[slot]
    routed = jnp.sum(route_weight[:, :, None] * picked.astype(jnp.float32), axis=1)
    shared_out = jnp.dot(shared_hidden, shared_down, preferred_element_type=jnp.float32)
    return (shared_out + routed).astype(jnp.bfloat16)


MESH = pl.DeviceIdType.MESH
BF = jnp.bfloat16
F32 = jnp.float32
PARTS = 2
AROUND = (3, 1, 2, 0)


def dot(a, b):
    return jnp.dot(a, b, preferred_element_type=F32)


def layer_kernel(
    n_dp, n_e, cap, groups,
    x_hbm, cur_hbm, ids_hbm, w_hbm, gate_hbm, up_hbm, down_hbm, sg_hbm, su_hbm, sd_hbm,
    out_ref,
    gu_v, down_v, sgu_v, sd_v, ids_v, w_v, flip, xm, cm,
    xc, part, rs_in, hid, acc, shv, sh_part, sh_in, sh_hid, own_sum, contrib, pair_in, fin_out, fin_in,
    in_sem, gu_sem, down_sem, shw_sem,
    snd, x_r, xp_r, cp_r, rs_s, rs_r, hid_s, hid_r, shp_r, shh_r, pair_r, fin_r,
):
    me_d = lax.axis_index("dp")
    me_e = lax.axis_index("expert")
    zs = n_e // 2
    z, c = me_e // 2, lax.rem(me_e, 2)
    pairs = zs // 2
    p, b = z // 2, lax.rem(z, 2)
    partner = 2 * z + (1 - c)
    tokens, width = x_hbm.shape
    top = ids_hbm.shape[0]
    chunk = gu_v.shape[2] // 2
    hs = chunk * PARTS
    shc = sgu_v.shape[2] // 2
    held = 2 * tokens
    slots = [(q, s) for q in range(PARTS) for s in AROUND]
    place_of = {slot: i for i, slot in enumerate(slots)}

    def start(src, dst, sem):
        copy = pltpu.make_async_copy(src, dst, sem)
        copy.start()
        return copy

    def landed(dst, sem):
        pltpu.make_async_copy(dst, dst, sem).wait()

    ys = n_dp // 2
    y, x = me_d // 2, lax.rem(me_d, 2)
    to_dp = [2 * lax.rem(y + s // 2, ys) + lax.rem(x + s % 2, 2) for s in range(n_dp)]
    from_dp = [2 * lax.rem(y - s // 2 + ys, ys) + lax.rem(x + s % 2, 2) for s in range(n_dp)]
    to_z = [2 * (2 * lax.rem(p + s // 2, pairs) + lax.rem(b + s % 2, 2)) + c for s in range(zs)]
    from_z = [2 * (2 * lax.rem(p - s // 2 + pairs, pairs) + lax.rem(b + s % 2, 2)) + c for s in range(zs)]

    def dp_dev(s):
        return to_dp[s]

    def dp_src(s):
        return from_dp[s]

    def z_dev(s):
        return to_z[s]

    def z_src(s):
        return from_z[s]

    barrier = pltpu.get_barrier_semaphore()
    pl.semaphore_signal(barrier, inc=1, device_id=(me_d, partner), device_id_type=MESH)
    for s in range(1, zs):
        pl.semaphore_signal(barrier, inc=1, device_id=(me_d, z_dev(s)), device_id_type=MESH)
    for s in range(1, n_dp):
        pl.semaphore_signal(barrier, inc=1, device_id=(dp_dev(s), me_e), device_id_type=MESH)

    got_ids = start(ids_hbm, ids_v, in_sem.at[0])
    got_w = start(w_hbm, w_v, in_sem.at[1])
    got_x = start(x_hbm, xm.at[c, :, pl.ds(0, width)], in_sem.at[2])
    got_cur = start(cur_hbm, cm.at[c], in_sem.at[3])
    def shared_at(d):
        return pl.ds(pl.multiple_of((c * n_dp + d) * shc, 128), shc)

    def fetch_shared():
        for i, s in enumerate(AROUND):
            start(sg_hbm.at[:, shared_at(dp_dev(s))], sgu_v.at[i, :, pl.ds(0, shc)], shw_sem.at[i])
            start(su_hbm.at[:, shared_at(dp_dev(s))], sgu_v.at[i, :, pl.ds(shc, shc)], shw_sem.at[i])

    def fetch_down():
        for q in range(PARTS):
            for i, s in enumerate([*range(n_dp - 1, 0, -1), 0]):
                row = pl.ds(pl.multiple_of(dp_src(s) * hs + q * chunk, 128), chunk)
                start(down_hbm.at[0, row, :], down_v.at[pl.ds((q * n_dp + i) * chunk, chunk), :], down_sem.at[q])

        for i, s in enumerate([*range(n_dp - 1, 0, -1), 0]):
            start(sd_hbm.at[shared_at(dp_src(s)), :], sd_v.at[pl.ds(i * shc, shc), :], shw_sem.at[n_dp])

    def remote(src, dst, ssem, rsem, dp, e):
        pltpu.make_async_remote_copy(
            src_ref=src, dst_ref=dst, send_sem=ssem, recv_sem=rsem, device_id=(dp, e), device_id_type=MESH
        ).start()

    before = lax.broadcasted_iota(jnp.int32, (128, 128), 0) < lax.broadcasted_iota(jnp.int32, (128, 128), 1)
    before = jnp.where(before, 1.0, 0.0).astype(BF)
    flip[...] = jnp.zeros_like(flip)
    for buf in xc:
        buf[...] = jnp.zeros_like(buf)
    got_ids.wait()
    got_w.wait()
    flip[:top, :tokens] = ids_v[...].astype(F32)
    flip[top:2 * top, :tokens] = w_v[...]
    named = flip[...]
    named = jnp.where(c == 1, pltpu.roll(named, tokens, 1), named)
    flip[...] = named
    exact = flip[top:2 * top, :]
    first = exact.astype(BF).astype(F32)
    second = (exact - first).astype(BF).astype(F32)
    flip[top:2 * top, :] = first
    flip[2 * top:3 * top, :] = second
    flip[3 * top:4 * top, :] = exact - first - second
    xm[c, :, width:] = flip[...].astype(BF)
    got_x.wait()
    got_cur.wait()
    for i, (q, s) in enumerate(slots):
        col = pl.ds(pl.multiple_of(dp_dev(s) * hs + q * chunk, 128), chunk)
        start(gate_hbm.at[0, :, col], gu_v.at[i, :, pl.ds(0, chunk)], gu_sem.at[i])
        start(up_hbm.at[0, :, col], gu_v.at[i, :, pl.ds(chunk, chunk)], gu_sem.at[i])
    with jax.named_scope("barrier"):
        pl.semaphore_wait(barrier, n_dp - 1 + zs - 1 + 1)

    remote(xm.at[c], xm.at[c], snd.at[0], xp_r.at[0], me_d, partner)
    for g in groups[1:]:
        for s in g:
            remote(xm.at[c], xm.at[2 * s + c], snd.at[0], x_r.at[s], me_d, z_dev(s))
    remote(cm.at[c], cm.at[c], snd.at[1], cp_r.at[0], me_d, partner)

    def relay_x(s):
        with jax.named_scope(f"relay{s}"):
            landed(xm.at[2 * s + c], x_r.at[s])
        remote(xm.at[2 * s + c], xm.at[2 * s + c], snd.at[0], xp_r.at[s], me_d, partner)

    me_f = me_e.astype(F32)

    def chosen(block):
        table = xm[block, :, width:].astype(F32)
        weight = table[top:2 * top] + table[2 * top:3 * top] + table[3 * top:4 * top]
        return jnp.sum(jnp.where(table[:top] == me_f, weight, 0.0), axis=0, keepdims=True)

    def route(g):
        rows = part[g].shape[1]
        padded = -(-rows // 16) * 16
        for s in groups[g]:
            with jax.named_scope(f"coll{s}"):
                landed(xm.at[2 * s + 1 - c], xp_r.at[s])
        scale = None
        for k, s in enumerate(groups[g]):
            one = chosen(2 * s) + chosen(2 * s + 1)
            one = pltpu.roll(one, held * k, 1) if k else one
            scale = one if scale is None else scale + one
        scale = jnp.broadcast_to(scale, (8, 128))
        rank = dot(jnp.where(scale > 0, 1.0, 0.0).astype(BF), before)[:1]
        scale = scale[:1]
        place = lax.broadcasted_iota(jnp.int32, (padded, 128), 0).astype(F32)
        place = jnp.where(jnp.logical_and(place == rank, scale > 0), 1.0, 0.0)
        size = held * len(groups[g])
        source = jnp.concatenate([xm[2 * s:2 * s + 2, :, :width].reshape(held, width) for s in groups[g]], axis=0)
        xc[g][:padded] = dot(place[:, :size].astype(BF), source).astype(BF)
        return place, scale

    def gate_up(g, hooks):
        rows = part[g].shape[1]
        value = None

        def ship(i, value):
            q, s = slots[i]
            part[g][i] = value[:rows].astype(BF)
            if s:
                remote(part[g].at[i], rs_in[g].at[q * (n_dp - 1) + s - 1], rs_s.at[g], rs_r.at[PARTS * g + q], dp_dev(s), me_e)

        for i in range(len(slots)):
            if g == 0:
                landed(gu_v.at[i], gu_sem.at[i])
            following = dot(xc[g][...], gu_v[i])
            if not DEFER:
                ship(i, following)
            elif i:
                ship(i - 1, value)
            value = following
            for hook in hooks.get(i, ()):
                hook()
        if DEFER:
            ship(len(slots) - 1, value)

    def back(g, place, scale):
        rows = part[g].shape[1]
        size = held * len(groups[g])
        tall = jnp.concatenate([place, jnp.zeros((128 - place.shape[0], 128), F32)], axis=0)
        turned = jnp.transpose(tall)[:size]
        weight = jnp.sum(place[:rows] * scale, axis=1, keepdims=True)
        return turned[:, :rows].astype(BF), weight

    def gated(term, n):
        gate, upper = term[:, :n], term[:, n:]
        return (gate / (1.0 + jnp.exp(-gate)) * upper).astype(BF)

    def act(g, q):
        base = q * n_dp
        with jax.named_scope(f"rs{g}{q}"):
            landed(rs_in[g].at[pl.ds(q * (n_dp - 1), n_dp - 1)], rs_r.at[PARTS * g + q])
        term = part[g][place_of[q, 0]].astype(F32)
        for s in range(1, n_dp):
            term = term + rs_in[g][q * (n_dp - 1) + s - 1].astype(F32)
        own = base + n_dp - 1
        hid[g][own] = gated(term, chunk)
        for s in range(1, n_dp):
            remote(hid[g].at[own], hid[g].at[base + n_dp - 1 - s], hid_s.at[g], hid_r.at[PARTS * g + q], dp_dev(s), me_e)

    span = n_dp * chunk
    half = width // HALVES

    def gathered(g, q):
        with jax.named_scope(f"hid{g}{q}"):
            landed(hid[g].at[pl.ds(q * n_dp, n_dp - 1)], hid_r.at[PARTS * g + q])
        if g == 1:
            landed(down_v.at[pl.ds(q * span, span), :], down_sem.at[q])
        return [hid[g][q * n_dp + i] for i in range(n_dp)]

    def down(g, weight):
        pieces = [piece for q in range(PARTS) for piece in gathered(g, q)]
        return (weight * dot(jnp.concatenate(pieces, axis=1), down_v[...])).astype(BF)

    def down_first(g):
        acc[...] = dot(jnp.concatenate(gathered(g, 0), axis=1), down_v[:span])

    def down_rest(g):
        return jnp.concatenate(gathered(g, 1), axis=1)

    def give(g, turned, value, h=None):
        cols = slice(0, width) if h is None else slice(h * half, (h + 1) * half)
        value = dot(turned, value)
        for k, s in enumerate(groups[g]):
            one = value[k * held:(k + 1) * held]
            if s == 0:
                one = one + shv[...]
            one = one.astype(BF).reshape(2, tokens, -1)
            for j in range(HALVES) if h is None else (h,):
                contrib[s, j] = one[:, :, j * half:(j + 1) * half] if h is None else one
                remote(contrib.at[s, j, 1 - c], pair_in.at[s, j], snd.at[4], pair_r.at[HALVES * s + j], me_d, partner)

    def settle(s, j):
        with jax.named_scope(f"pair{s}{j}"):
            landed(pair_in.at[s, j], pair_r.at[HALVES * s + j])
        summed = contrib[s, j, c].astype(F32) + pair_in[s, j].astype(F32)
        if s:
            fin_out[s - 1, j] = summed.astype(BF)
            remote(fin_out.at[s - 1, j], fin_in.at[s - 1, j], snd.at[5], fin_r.at[HALVES * s + j], me_d, z_src(s))
        else:
            own_sum[:, j * half:(j + 1) * half] = summed

    def shared_up(lo, hi):
        if lo == 0:
            with jax.named_scope("ccoll"):
                landed(cm.at[1 - c], cp_r.at[0])
        cur = cm[...].reshape(held, width)
        value = None

        def ship(i, value):
            s = AROUND[i]
            sh_part[i] = value.astype(BF)
            if s:
                remote(sh_part.at[i], sh_in.at[s - 1], snd.at[2], shp_r.at[0], dp_dev(s), me_e)

        for i in range(lo, hi):
            with jax.named_scope(f"shw{i}"):
                landed(sgu_v.at[i], shw_sem.at[i])
            following = dot(cur, sgu_v[i])
            if i > lo:
                ship(i - 1, value)
            value = following
        ship(hi - 1, value)

    def shared_act():
        with jax.named_scope("shrs"):
            landed(sh_in, shp_r.at[0])
        term = sh_part[n_dp - 1].astype(F32)
        for s in range(1, n_dp):
            term = term + sh_in[s - 1].astype(F32)
        sh_hid[n_dp - 1] = gated(term, shc)
        for s in range(1, n_dp):
            remote(sh_hid.at[n_dp - 1], sh_hid.at[n_dp - 1 - s], snd.at[3], shh_r.at[0], dp_dev(s), me_e)

    def shared_down():
        with jax.named_scope("shh"):
            landed(sh_hid.at[pl.ds(0, n_dp - 1)], shh_r.at[0])
        landed(sd_v, shw_sem.at[n_dp])
        shv[...] = dot(jnp.concatenate([sh_hid[i] for i in range(n_dp)], axis=1), sd_v[...])

    order = list(range(len(groups)))
    kept = {}

    def do(*calls):
        return [functools.partial(*call) for call in calls]

    hooks = [
        {0: do((fetch_shared,)), 3: do((fetch_down,)), 6: do((relay_x, 1))},
        {2: do((relay_x, 3))},
        {1: do((relay_x, 2))},
        {2: do((act, 1, 1))},
    ]
    for g in order:
        place, scale = route(g)
        gate_up(g, hooks[g])
        kept[g] = back(g, place, scale)
        if g == 0:
            shared_up(0, 2)
        if g == 2:
            act(1, 0)
    act(2, 0)
    act(2, 1)
    shared_up(2, n_dp)
    act(3, 0)
    act(3, 1)
    act(0, 0)
    act(0, 1)
    give(1, kept[1][0], down(1, kept[1][1]))
    give(2, kept[2][0], down(2, kept[2][1]))
    shared_act()
    down_first(3)
    for j in range(HALVES):
        settle(1, j)
    for j in range(HALVES):
        settle(3, j)
    lhs = down_rest(3)
    turned, weight = kept[3]
    for j in range(HALVES):
        cols = slice(j * half, (j + 1) * half)
        value = acc[:, cols] + dot(lhs, down_v[span:, cols])
        give(3, turned, (weight * value).astype(BF), j)
    for j in range(HALVES):
        settle(2, j)
    shared_down()
    give(0, kept[0][0], down(0, kept[0][1]))
    for j in range(HALVES):
        settle(0, j)
    for j in range(HALVES):
        cols = slice(j * half, (j + 1) * half)
        both = own_sum[:, cols]
        for s in range(1, zs):
            with jax.named_scope(f"fin{s}{j}"):
                landed(fin_in.at[s - 1, j], fin_r.at[HALVES * s + j])
            both = both + fin_in[s - 1, j].astype(F32)
        out_ref[:, cols] = both.astype(BF)

    def sent(ref, sem):
        pltpu.make_async_remote_copy(
            src_ref=ref, dst_ref=ref, send_sem=sem, recv_sem=sem, device_id=(me_d, partner), device_id_type=MESH
        ).wait_send()

    with jax.named_scope("sendwait"):
        sent(xm.at[pl.ds(0, 2 * zs - 1)], snd.at[0])
        sent(cm.at[0], snd.at[1])
        sent(sh_part.at[pl.ds(0, n_dp - 1)], snd.at[2])
        sent(sh_hid.at[pl.ds(0, n_dp - 1)], snd.at[3])
        sent(pair_in, snd.at[4])
        sent(fin_out, snd.at[5])
        for g in order:
            sent(part[g].at[pl.ds(0, PARTS * (n_dp - 1))], rs_s.at[g])
            sent(hid[g].at[pl.ds(0, PARTS * (n_dp - 1))], hid_s.at[g])


GROUPS = ((0,), (1,), (3,), (2,))
HALVES = 1
DEFER = True


def fused(n_dp, n_e, shortcut_in, current_in, expert_ids, route_weight, gate_weight, up_weight, down_weight, shared_gate, shared_up, shared_down):
    tokens, width = shortcut_in.shape
    hidden = gate_weight.shape[2]
    top = expert_ids.shape[1]
    cap = 3 * tokens * top // (2 * n_e)
    chunk = hidden // n_dp // PARTS
    count = PARTS * n_dp
    zs = n_e // 2
    shc = hidden // (2 * n_dp)
    held = 2 * tokens
    rows = [2 * cap * len(g) for g in GROUPS]
    n_g = len(GROUPS)
    V = pltpu.VMEM
    S = pltpu.SemaphoreType.DMA
    scratch = [
        V((count, width, 2 * chunk), BF), V((hidden, width), BF), V((n_dp, width, 2 * shc), BF), V((n_dp * shc, width), BF),
        V((top, tokens), jnp.int32), V((top, tokens), F32), V((tokens, 128), F32),
        V((n_e, tokens, width + 128), BF), V((2, tokens, width), BF),
        [V((128, width), BF) for r in rows], [V((count, r, 2 * chunk), BF) for r in rows],
        [V((PARTS * (n_dp - 1), r, 2 * chunk), BF) for r in rows], [V((count, r, chunk), BF) for r in rows],
        V((rows[-1], width), F32), V((held, width), F32),
        V((n_dp, held, 2 * shc), BF), V((n_dp - 1, held, 2 * shc), BF), V((n_dp, held, shc), BF), V((tokens, width), F32),
        V((zs, HALVES, 2, tokens, width // HALVES), BF), V((zs, HALVES, tokens, width // HALVES), BF),
        *[V((zs - 1, HALVES, tokens, width // HALVES), BF) for _ in range(2)],
        S((4,)), S((count,)), S((PARTS,)), S((n_dp + 1,)),
        S((6,)), S((zs,)), S((zs,)), S((1,)),
        S((n_g,)), S((PARTS * n_g,)), S((n_g,)), S((PARTS * n_g,)), S((1,)), S((1,)), S((HALVES * zs,)), S((HALVES * zs,)),
    ]
    vm = pl.BlockSpec(memory_space=pltpu.VMEM)
    hbm = pl.BlockSpec(memory_space=pl.ANY)
    return pl.pallas_call(
        functools.partial(layer_kernel, n_dp, n_e, cap, GROUPS),
        out_shape=pltpu.VMEM((tokens, width), BF),
        in_specs=[hbm] * 10,
        out_specs=vm,
        scratch_shapes=scratch,
        compiler_params=pltpu.CompilerParams(collective_id=0, has_side_effects=True, vmem_limit_bytes=60 * 1024 * 1024),
    )(shortcut_in, current_in, expert_ids.T, route_weight.T, gate_weight, up_weight, down_weight, shared_gate, shared_up, shared_down)


def body(n_dp, n_e, *arrays):
    tokens, width = arrays[0].shape
    top = arrays[2].shape[1]
    experts, _, hidden = arrays[4].shape
    aligned = (
        experts == 1 and n_dp == 4 and n_e == 2 * sum(len(g) for g in GROUPS) and 4 * top <= tokens and tokens == 16 and width % (HALVES * 128) == 0
        and hidden % (n_dp * PARTS * 128) == 0 and hidden % (2 * n_dp * 128) == 0
        and 3 * tokens * top % (2 * n_e) == 0 and 2 * (3 * tokens * top // (2 * n_e)) % 8 == 0
    )
    return fused(n_dp, n_e, *arrays) if aligned else local(*arrays)


def solution(mesh):
    placed = (
        P("expert", "dp"),
        P("expert", "dp"),
        P("expert", None),
        P("expert", None),
        P("expert", "dp", None),
        P("expert", "dp", None),
        P("expert", None, "dp"),
        P("dp", None),
        P("dp", None),
        P(None, "dp"),
    )
    return jax.shard_map(
        functools.partial(body, mesh.shape["dp"], mesh.shape["expert"]), mesh=mesh, in_specs=placed, out_specs=P("expert", "dp"), check_vma=False
    )
```

```python
import functools

import jax
import jax.numpy as jnp
from jax import lax
from jax.experimental import pallas as pl
from jax.experimental.pallas import tpu as pltpu
from jax.sharding import PartitionSpec as P


def activate(summed):
    return (jax.nn.silu(summed[:, 0]) * summed[:, 1]).astype(jnp.bfloat16)


def hidden_of(partial_value):
    summed = lax.psum_scatter(
        partial_value.astype(jnp.bfloat16), "dp", scatter_dimension=2, tiled=True
    ).astype(jnp.float32)
    return lax.all_gather(activate(summed), "dp", axis=1, tiled=True)


def send_rows(outgoing):
    return lax.all_to_all(outgoing, "expert", split_axis=0, concat_axis=0, tiled=True)


def expert_partial(arrived, gate_weight, up_weight):
    gate = jnp.einsum("sacd,adh->sach", arrived, gate_weight, preferred_element_type=jnp.float32)
    upper = jnp.einsum("sacd,adh->sach", arrived, up_weight, preferred_element_type=jnp.float32)
    stacked = jnp.stack([gate, upper], axis=3)
    return stacked.reshape(-1, 2, gate_weight.shape[2])


def local(
    shortcut_in,
    current_in,
    expert_ids,
    route_weight,
    gate_weight,
    up_weight,
    down_weight,
    shared_gate,
    shared_up,
    shared_down,
):
    sources = lax.axis_size("expert")
    local_experts = gate_weight.shape[0]
    experts = sources * local_experts
    tokens, top = expert_ids.shape
    capacity = 3 * tokens * top // (2 * experts)
    width = shortcut_in.shape[1]
    hidden_units = gate_weight.shape[2]
    flat_ids = expert_ids.reshape(-1)
    onehot = (flat_ids[:, None] == jnp.arange(experts, dtype=jnp.int32)[None, :]).astype(jnp.int32)
    rank = jnp.sum((jnp.cumsum(onehot, axis=0) - 1) * onehot, axis=1)
    slot = (flat_ids * capacity + rank).reshape(tokens, top)
    positions = jnp.arange(experts * capacity, dtype=jnp.int32)
    place = jnp.sum((slot[None, :, :] == positions[:, None, None]).astype(jnp.bfloat16), axis=2)
    outgoing = jnp.dot(place, shortcut_in, preferred_element_type=jnp.float32).astype(jnp.bfloat16)
    outgoing = outgoing.reshape(sources, local_experts * capacity, width)
    shared_gate_sum = jnp.dot(current_in, shared_gate, preferred_element_type=jnp.float32)
    shared_up_sum = jnp.dot(current_in, shared_up, preferred_element_type=jnp.float32)
    shared_partial = jnp.stack([shared_gate_sum, shared_up_sum], axis=1)
    routed_rows = experts * capacity
    arrived = send_rows(outgoing).reshape(sources, local_experts, capacity, width)
    routed_partial = expert_partial(arrived, gate_weight, up_weight)
    joined = hidden_of(jnp.concatenate([routed_partial, shared_partial], axis=0))
    routed_hidden = joined[:routed_rows]
    shared_hidden = joined[routed_rows:]
    routed_hidden = routed_hidden.reshape(sources, local_experts, capacity, hidden_units)
    expert_out = jnp.einsum(
        "sach,ahd->sacd", routed_hidden, down_weight, preferred_element_type=jnp.float32
    ).astype(jnp.bfloat16)
    returned = lax.all_to_all(
        expert_out.reshape(sources, local_experts * capacity, width),
        "expert",
        split_axis=0,
        concat_axis=0,
        tiled=True,
    )
    picked = returned.reshape(routed_rows, width)[slot]
    routed = jnp.sum(route_weight[:, :, None] * picked.astype(jnp.float32), axis=1)
    shared_out = jnp.dot(shared_hidden, shared_down, preferred_element_type=jnp.float32)
    return (shared_out + routed).astype(jnp.bfloat16)


MESH = pl.DeviceIdType.MESH
BF = jnp.bfloat16
F32 = jnp.float32
PARTS = 2
AROUND = (3, 1, 2, 0)


def dot(a, b):
    return jnp.dot(a, b, preferred_element_type=F32)


def layer_kernel(
    n_dp, n_e, cap, groups,
    x_hbm, cur_hbm, ids_hbm, w_hbm, gate_hbm, up_hbm, down_hbm, sg_hbm, su_hbm, sd_hbm,
    out_ref,
    gu_v, down_v, sgu_v, sd_v, ids_v, w_v, flip, xm, cm,
    xc, part, rs_in, hid, acc, shv, sh_part, sh_in, sh_hid, own_sum, contrib, pair_in, fin_out, fin_in,
    in_sem, gu_sem, down_sem, shw_sem,
    snd, x_r, xp_r, cp_r, rs_s, rs_r, hid_s, hid_r, shp_r, shh_r, pair_r, fin_r,
):
    me_d = lax.axis_index("dp")
    me_e = lax.axis_index("expert")
    zs = n_e // 2
    z, c = me_e // 2, lax.rem(me_e, 2)
    pairs = zs // 2
    p, b = z // 2, lax.rem(z, 2)
    partner = 2 * z + (1 - c)
    tokens, width = x_hbm.shape
    top = ids_hbm.shape[0]
    chunk = gu_v.shape[2] // 2
    hs = chunk * PARTS
    shc = sgu_v.shape[2] // 2
    held = 2 * tokens
    named_rows = -(-n_e // 16) * 16
    slots = [(q, s) for q in range(PARTS) for s in AROUND]
    place_of = {slot: i for i, slot in enumerate(slots)}

    def start(src, dst, sem):
        copy = pltpu.make_async_copy(src, dst, sem)
        copy.start()
        return copy

    def landed(dst, sem):
        pltpu.make_async_copy(dst, dst, sem).wait()

    ys = n_dp // 2
    y, x = me_d // 2, lax.rem(me_d, 2)
    to_dp = [2 * lax.rem(y + s // 2, ys) + lax.rem(x + s % 2, 2) for s in range(n_dp)]
    from_dp = [2 * lax.rem(y - s // 2 + ys, ys) + lax.rem(x + s % 2, 2) for s in range(n_dp)]
    to_z = [2 * (2 * lax.rem(p + s // 2, pairs) + lax.rem(b + s % 2, 2)) + c for s in range(zs)]
    from_z = [2 * (2 * lax.rem(p - s // 2 + pairs, pairs) + lax.rem(b + s % 2, 2)) + c for s in range(zs)]

    def dp_dev(s):
        return to_dp[s]

    def dp_src(s):
        return from_dp[s]

    def z_dev(s):
        return to_z[s]

    def z_src(s):
        return from_z[s]

    barrier = pltpu.get_barrier_semaphore()
    pl.semaphore_signal(barrier, inc=1, device_id=(me_d, partner), device_id_type=MESH)
    for s in range(1, zs):
        pl.semaphore_signal(barrier, inc=1, device_id=(me_d, z_dev(s)), device_id_type=MESH)
    for s in range(1, n_dp):
        pl.semaphore_signal(barrier, inc=1, device_id=(dp_dev(s), me_e), device_id_type=MESH)

    got_ids = start(ids_hbm, ids_v, in_sem.at[0])
    got_w = start(w_hbm, w_v, in_sem.at[1])
    got_x = start(x_hbm, xm.at[c, :, pl.ds(0, width)], in_sem.at[2])
    got_cur = start(cur_hbm, cm.at[c], in_sem.at[3])
    def shared_at(d):
        return pl.ds(pl.multiple_of((c * n_dp + d) * shc, 128), shc)

    def fetch_shared():
        for i, s in enumerate(AROUND):
            start(sg_hbm.at[:, shared_at(dp_dev(s))], sgu_v.at[i, :, pl.ds(0, shc)], shw_sem.at[i])
            start(su_hbm.at[:, shared_at(dp_dev(s))], sgu_v.at[i, :, pl.ds(shc, shc)], shw_sem.at[i])

    def fetch_down():
        for q in range(PARTS):
            for i, s in enumerate([*range(n_dp - 1, 0, -1), 0]):
                row = pl.ds(pl.multiple_of(dp_src(s) * hs + q * chunk, 128), chunk)
                start(down_hbm.at[0, row, :], down_v.at[pl.ds((q * n_dp + i) * chunk, chunk), :], down_sem.at[q])

        for i, s in enumerate([*range(n_dp - 1, 0, -1), 0]):
            start(sd_hbm.at[shared_at(dp_src(s)), :], sd_v.at[pl.ds(i * shc, shc), :], shw_sem.at[n_dp])

    def remote(src, dst, ssem, rsem, dp, e):
        pltpu.make_async_remote_copy(
            src_ref=src, dst_ref=dst, send_sem=ssem, recv_sem=rsem, device_id=(dp, e), device_id_type=MESH
        ).start()

    before = lax.broadcasted_iota(jnp.int32, (128, 128), 0) < lax.broadcasted_iota(jnp.int32, (128, 128), 1)
    before = jnp.where(before, 1.0, 0.0).astype(BF)
    flip[...] = jnp.zeros_like(flip)
    for buf in xc:
        buf[...] = jnp.zeros_like(buf)
    got_ids.wait()
    got_w.wait()
    ids = ids_v[...].astype(F32)
    flip[:top, :tokens] = ids
    numbers = lax.broadcasted_iota(jnp.int32, (named_rows, 128), 0).astype(F32)
    spread_ids = flip[:top, :]
    inside = lax.broadcasted_iota(jnp.int32, (named_rows, 128), 1) < tokens
    taken = jnp.zeros((named_rows, 128), F32)
    for k in range(top):
        taken = taken + jnp.where(jnp.logical_and(spread_ids[k:k + 1] == numbers, inside), 1.0, 0.0)
    ranks = dot(taken.astype(BF), before)
    for k in range(top):
        rank = jnp.sum(jnp.where(spread_ids[k:k + 1] == numbers, ranks, 0.0), axis=0, keepdims=True)
        flip[k:k + 1, :] = spread_ids[k:k + 1] * STRIDE + rank
    flip[top:2 * top, :tokens] = w_v[...]
    named = flip[...]
    named = jnp.where(c == 1, pltpu.roll(named, tokens, 1), named)
    flip[...] = named
    exact = flip[top:2 * top, :]
    first = exact.astype(BF).astype(F32)
    second = (exact - first).astype(BF).astype(F32)
    flip[top:2 * top, :] = first
    flip[2 * top:3 * top, :] = second
    flip[3 * top:4 * top, :] = exact - first - second
    xm[c, :, width:] = flip[...].astype(BF)
    got_x.wait()
    got_cur.wait()
    for i, (q, s) in enumerate(slots):
        col = pl.ds(pl.multiple_of(dp_dev(s) * hs + q * chunk, 128), chunk)
        start(gate_hbm.at[0, :, col], gu_v.at[i, :, pl.ds(0, chunk)], gu_sem.at[i])
        start(up_hbm.at[0, :, col], gu_v.at[i, :, pl.ds(chunk, chunk)], gu_sem.at[i])
    with jax.named_scope("barrier"):
        pl.semaphore_wait(barrier, n_dp - 1 + zs - 1 + 1)

    remote(xm.at[c], xm.at[c], snd.at[0], xp_r.at[0], me_d, partner)
    for g in groups[1:]:
        for s in g:
            remote(xm.at[c], xm.at[2 * s + c], snd.at[0], x_r.at[s], me_d, z_dev(s))
    remote(cm.at[c], cm.at[c], snd.at[1], cp_r.at[0], me_d, partner)

    def relay_x(s):
        with jax.named_scope(f"relay{s}"):
            landed(xm.at[2 * s + c], x_r.at[s])
        remote(xm.at[2 * s + c], xm.at[2 * s + c], snd.at[0], xp_r.at[s], me_d, partner)

    me_f = me_e.astype(F32)

    def chosen(block):
        table = xm[block, :, width:].astype(F32)
        weight = table[top:2 * top] + table[2 * top:3 * top] + table[3 * top:4 * top]
        offset = table[:top] - me_f * STRIDE
        mine = jnp.logical_and(jnp.logical_and(offset >= 0, offset < STRIDE), weight > 0)
        scale = jnp.sum(jnp.where(mine, weight, 0.0), axis=0, keepdims=True)
        return scale, jnp.sum(jnp.where(mine, offset + (block % 2) * cap, 0.0), axis=0, keepdims=True)

    def route(g):
        rows = part[g].shape[1]
        padded = -(-rows // 16) * 16
        for s in groups[g]:
            with jax.named_scope(f"coll{s}"):
                landed(xm.at[2 * s + 1 - c], xp_r.at[s])
        scale = rank = None
        for k, s in enumerate(groups[g]):
            pair = [chosen(2 * s), chosen(2 * s + 1)]
            one = [pair[0][n] + pair[1][n] for n in (0, 1)]
            one[1] = one[1] + jnp.where(one[0] > 0, 2 * cap * k, 0.0) if k else one[1]
            one = [pltpu.roll(row, held * k, 1) for row in one] if k else one
            scale, rank = one if scale is None else (scale + one[0], rank + one[1])
        place = lax.broadcasted_iota(jnp.int32, (padded, 128), 0).astype(F32)
        place = jnp.where(jnp.logical_and(place == rank, scale > 0), 1.0, 0.0)
        size = held * len(groups[g])
        source = jnp.concatenate([xm[2 * s:2 * s + 2, :, :width].reshape(held, width) for s in groups[g]], axis=0)
        xc[g][:padded] = dot(place[:, :size].astype(BF), source).astype(BF)
        return place, scale

    def gate_up(g, hooks):
        rows = part[g].shape[1]
        value = None

        def ship(i, value):
            q, s = slots[i]
            part[g][i] = value[:rows].astype(BF)
            if s:
                remote(part[g].at[i], rs_in[g].at[q * (n_dp - 1) + s - 1], rs_s.at[g], rs_r.at[PARTS * g + q], dp_dev(s), me_e)

        for i in range(len(slots)):
            if g == 0:
                landed(gu_v.at[i], gu_sem.at[i])
            following = dot(xc[g][...], gu_v[i])
            if not DEFER:
                ship(i, following)
            elif i:
                ship(i - 1, value)
            value = following
            for hook in hooks.get(i, ()):
                hook()
        if DEFER:
            ship(len(slots) - 1, value)

    def back(g, place, scale):
        rows = part[g].shape[1]
        size = held * len(groups[g])
        tall = jnp.concatenate([place, jnp.zeros((128 - place.shape[0], 128), F32)], axis=0)
        turned = jnp.transpose(tall)[:size]
        weight = jnp.sum(place[:rows] * scale, axis=1, keepdims=True)
        return turned[:, :rows].astype(BF), weight

    def gated(term, n):
        gate, upper = term[:, :n], term[:, n:]
        return (gate / (1.0 + jnp.exp(-gate)) * upper).astype(BF)

    def act(g, q):
        base = q * n_dp
        with jax.named_scope(f"rs{g}{q}"):
            landed(rs_in[g].at[pl.ds(q * (n_dp - 1), n_dp - 1)], rs_r.at[PARTS * g + q])
        term = part[g][place_of[q, 0]].astype(F32)
        for s in range(1, n_dp):
            term = term + rs_in[g][q * (n_dp - 1) + s - 1].astype(F32)
        own = base + n_dp - 1
        hid[g][own] = gated(term, chunk)
        for s in range(1, n_dp):
            remote(hid[g].at[own], hid[g].at[base + n_dp - 1 - s], hid_s.at[g], hid_r.at[PARTS * g + q], dp_dev(s), me_e)

    span = n_dp * chunk
    half = width // HALVES

    def gathered(g, q):
        with jax.named_scope(f"hid{g}{q}"):
            landed(hid[g].at[pl.ds(q * n_dp, n_dp - 1)], hid_r.at[PARTS * g + q])
        if g == 1:
            landed(down_v.at[pl.ds(q * span, span), :], down_sem.at[q])
        return [hid[g][q * n_dp + i] for i in range(n_dp)]

    def down(g, weight):
        pieces = [piece for q in range(PARTS) for piece in gathered(g, q)]
        return (weight * dot(jnp.concatenate(pieces, axis=1), down_v[...])).astype(BF)

    def down_first(g):
        acc[...] = dot(jnp.concatenate(gathered(g, 0), axis=1), down_v[:span])

    def down_rest(g):
        return jnp.concatenate(gathered(g, 1), axis=1)

    def give(g, turned, value, h=None):
        cols = slice(0, width) if h is None else slice(h * half, (h + 1) * half)
        value = dot(turned, value)
        for k, s in enumerate(groups[g]):
            one = value[k * held:(k + 1) * held]
            if s == 0:
                one = one + shv[...]
            one = one.astype(BF).reshape(2, tokens, -1)
            for j in range(HALVES) if h is None else (h,):
                contrib[s, j] = one[:, :, j * half:(j + 1) * half] if h is None else one
                remote(contrib.at[s, j, 1 - c], pair_in.at[s, j], snd.at[4], pair_r.at[HALVES * s + j], me_d, partner)

    def settle(s, j):
        with jax.named_scope(f"pair{s}{j}"):
            landed(pair_in.at[s, j], pair_r.at[HALVES * s + j])
        summed = contrib[s, j, c].astype(F32) + pair_in[s, j].astype(F32)
        if s:
            fin_out[s - 1, j] = summed.astype(BF)
            remote(fin_out.at[s - 1, j], fin_in.at[s - 1, j], snd.at[5], fin_r.at[HALVES * s + j], me_d, z_src(s))
        else:
            own_sum[:, j * half:(j + 1) * half] = summed

    def shared_up(lo, hi):
        if lo == 0:
            with jax.named_scope("ccoll"):
                landed(cm.at[1 - c], cp_r.at[0])
        cur = cm[...].reshape(held, width)
        value = None

        def ship(i, value):
            s = AROUND[i]
            sh_part[i] = value.astype(BF)
            if s:
                remote(sh_part.at[i], sh_in.at[s - 1], snd.at[2], shp_r.at[0], dp_dev(s), me_e)

        for i in range(lo, hi):
            with jax.named_scope(f"shw{i}"):
                landed(sgu_v.at[i], shw_sem.at[i])
            following = dot(cur, sgu_v[i])
            if i > lo:
                ship(i - 1, value)
            value = following
        ship(hi - 1, value)

    def shared_act():
        with jax.named_scope("shrs"):
            landed(sh_in, shp_r.at[0])
        term = sh_part[n_dp - 1].astype(F32)
        for s in range(1, n_dp):
            term = term + sh_in[s - 1].astype(F32)
        sh_hid[n_dp - 1] = gated(term, shc)
        for s in range(1, n_dp):
            remote(sh_hid.at[n_dp - 1], sh_hid.at[n_dp - 1 - s], snd.at[3], shh_r.at[0], dp_dev(s), me_e)

    def shared_down():
        with jax.named_scope("shh"):
            landed(sh_hid.at[pl.ds(0, n_dp - 1)], shh_r.at[0])
        landed(sd_v, shw_sem.at[n_dp])
        shv[...] = dot(jnp.concatenate([sh_hid[i] for i in range(n_dp)], axis=1), sd_v[...])

    order = list(range(len(groups)))
    kept = {}

    def do(*calls):
        return [functools.partial(*call) for call in calls]

    hooks = [
        {0: do((fetch_shared,)), 3: do((fetch_down,)), 6: do((relay_x, 1))},
        {2: do((relay_x, 3))},
        {1: do((relay_x, 2))},
        {1: do((act, 1, 0)), 3: do((act, 1, 1))},
    ]
    for g in order:
        place, scale = route(g)
        gate_up(g, hooks[g])
        kept[g] = back(g, place, scale)
        if g == 0:
            shared_up(0, 1)
    act(2, 0)
    act(2, 1)
    shared_up(1, n_dp)
    act(3, 0)
    act(3, 1)
    act(0, 0)
    act(0, 1)
    second_value = down(1, kept[1][1])
    give(2, kept[2][0], down(2, kept[2][1]))
    give(1, kept[1][0], second_value)
    shared_act()
    down_first(3)
    for j in range(HALVES):
        settle(3, j)
    for j in range(HALVES):
        settle(1, j)
    lhs = down_rest(3)
    turned, weight = kept[3]
    for j in range(HALVES):
        cols = slice(j * half, (j + 1) * half)
        value = acc[:, cols] + dot(lhs, down_v[span:, cols])
        give(3, turned, (weight * value).astype(BF), j)
    for j in range(HALVES):
        settle(2, j)
    shared_down()
    give(0, kept[0][0], down(0, kept[0][1]))
    for j in range(HALVES):
        settle(0, j)
    for j in range(HALVES):
        cols = slice(j * half, (j + 1) * half)
        both = own_sum[:, cols]
        for s in range(1, zs):
            with jax.named_scope(f"fin{s}{j}"):
                landed(fin_in.at[s - 1, j], fin_r.at[HALVES * s + j])
            both = both + fin_in[s - 1, j].astype(F32)
        out_ref[:, cols] = both.astype(BF)

    def sent(ref, sem):
        pltpu.make_async_remote_copy(
            src_ref=ref, dst_ref=ref, send_sem=sem, recv_sem=sem, device_id=(me_d, partner), device_id_type=MESH
        ).wait_send()

    with jax.named_scope("sendwait"):
        sent(xm.at[pl.ds(0, 2 * zs - 1)], snd.at[0])
        sent(cm.at[0], snd.at[1])
        sent(sh_part.at[pl.ds(0, n_dp - 1)], snd.at[2])
        sent(sh_hid.at[pl.ds(0, n_dp - 1)], snd.at[3])
        sent(pair_in, snd.at[4])
        sent(fin_out, snd.at[5])
        for g in order:
            sent(part[g].at[pl.ds(0, PARTS * (n_dp - 1))], rs_s.at[g])
            sent(hid[g].at[pl.ds(0, PARTS * (n_dp - 1))], hid_s.at[g])


GROUPS = ((0,), (1,), (3,), (2,))
HALVES = 1
STRIDE = 16
DEFER = True


def fused(n_dp, n_e, shortcut_in, current_in, expert_ids, route_weight, gate_weight, up_weight, down_weight, shared_gate, shared_up, shared_down):
    tokens, width = shortcut_in.shape
    hidden = gate_weight.shape[2]
    top = expert_ids.shape[1]
    cap = 3 * tokens * top // (2 * n_e)
    chunk = hidden // n_dp // PARTS
    count = PARTS * n_dp
    zs = n_e // 2
    shc = hidden // (2 * n_dp)
    held = 2 * tokens
    rows = [2 * cap * len(g) for g in GROUPS]
    n_g = len(GROUPS)
    V = pltpu.VMEM
    S = pltpu.SemaphoreType.DMA
    scratch = [
        V((count, width, 2 * chunk), BF), V((hidden, width), BF), V((n_dp, width, 2 * shc), BF), V((n_dp * shc, width), BF),
        V((top, tokens), jnp.int32), V((top, tokens), F32), V((tokens, 128), F32),
        V((n_e, tokens, width + 128), BF), V((2, tokens, width), BF),
        [V((128, width), BF) for r in rows], [V((count, r, 2 * chunk), BF) for r in rows],
        [V((PARTS * (n_dp - 1), r, 2 * chunk), BF) for r in rows], [V((count, r, chunk), BF) for r in rows],
        V((rows[-1], width), F32), V((held, width), F32),
        V((n_dp, held, 2 * shc), BF), V((n_dp - 1, held, 2 * shc), BF), V((n_dp, held, shc), BF), V((tokens, width), F32),
        V((zs, HALVES, 2, tokens, width // HALVES), BF), V((zs, HALVES, tokens, width // HALVES), BF),
        *[V((zs - 1, HALVES, tokens, width // HALVES), BF) for _ in range(2)],
        S((4,)), S((count,)), S((PARTS,)), S((n_dp + 1,)),
        S((6,)), S((zs,)), S((zs,)), S((1,)),
        S((n_g,)), S((PARTS * n_g,)), S((n_g,)), S((PARTS * n_g,)), S((1,)), S((1,)), S((HALVES * zs,)), S((HALVES * zs,)),
    ]
    vm = pl.BlockSpec(memory_space=pltpu.VMEM)
    hbm = pl.BlockSpec(memory_space=pl.ANY)
    return pl.pallas_call(
        functools.partial(layer_kernel, n_dp, n_e, cap, GROUPS),
        out_shape=pltpu.VMEM((tokens, width), BF),
        in_specs=[hbm] * 10,
        out_specs=vm,
        scratch_shapes=scratch,
        compiler_params=pltpu.CompilerParams(collective_id=0, has_side_effects=True, vmem_limit_bytes=60 * 1024 * 1024),
    )(shortcut_in, current_in, expert_ids.T, route_weight.T, gate_weight, up_weight, down_weight, shared_gate, shared_up, shared_down)


def body(n_dp, n_e, *arrays):
    tokens, width = arrays[0].shape
    top = arrays[2].shape[1]
    experts, _, hidden = arrays[4].shape
    aligned = (
        experts == 1 and n_dp == 4 and n_e == 2 * sum(len(g) for g in GROUPS) and 4 * top <= tokens and tokens == STRIDE and n_e * STRIDE <= 256 and width % (HALVES * 128) == 0
        and hidden % (n_dp * PARTS * 128) == 0 and hidden % (2 * n_dp * 128) == 0
        and 3 * tokens * top % (2 * n_e) == 0 and 2 * (3 * tokens * top // (2 * n_e)) % 8 == 0
    )
    return fused(n_dp, n_e, *arrays) if aligned else local(*arrays)


def solution(mesh):
    placed = (
        P("expert", "dp"),
        P("expert", "dp"),
        P("expert", None),
        P("expert", None),
        P("expert", "dp", None),
        P("expert", "dp", None),
        P("expert", None, "dp"),
        P("dp", None),
        P("dp", None),
        P(None, "dp"),
    )
    return jax.shard_map(
        functools.partial(body, mesh.shape["dp"], mesh.shape["expert"]), mesh=mesh, in_specs=placed, out_specs=P("expert", "dp"), check_vma=False
    )
```
